32 devices in a mesh: rep: 4 (over z), tm: 4 (over x, core), space: 2 (over y).
Axes of the slice: x: 2, y: 2, z: 4, core: 2. Of those that a mesh axis runs over, the one named last changes fastest.
Arguments:
- spins: float32 [20, 3, 64, 4096], P('rep', None, 'tm', 'space'), may hold values from -4 to 4
- bond_right: float32 [4096], P('space'), may hold values from -4 to 4
- bond_down: float32 [4096], P('space'), may hold values from -4 to 4
- betas: float32 [20], P('rep'), may hold values from 0.2 to 2
- time_coupling: float32 [20], P('rep'), may hold values from 0.1 to 1
- thresholds: int32 [2, 20, 64, 4096], P(None, 'rep', 'tm', 'space'), may hold values from 0 to 8191
- partner: int32 [20], P('rep'), may hold values from 0 to 19, as said below
- accept: int32 [20], P('rep'), may hold values from 0 to 1, as said below
Outputs:
- swapped: float32 [20, 3, 64, 4096], P('rep', None, 'tm', 'space')
- energies: float32 [20, 64], P('rep', 'tm')
The draws below stay inside these ranges and needn't reach their ends.
Inputs may be any that keep to these rules, and one draw needn't show every extreme that they name: partner[r] is r - 1, r or r + 1, and partner[partner[r]] = r; partner[r] = r + 1 wherever r % 5 = 4 and r + 1 < 20. accept[r] = accept[partner[r]], accept[r] = 0 where partner[r] = r, and accept[r] = 1 wherever r % 5 = 4 and r + 1 < 20.
All inputs are finite; a program needn't handle non-finite values.
Results may differ from the reference program's by a relative error of at most 0.0001.
Values sent between devices are 32-bit elements; how exact they have to be, the bound alone decides.
A program may use at most 64 MiB of HBM per device.

```python
import math
import jax
import jax.numpy as jnp
from jax import lax

REP_DEV = 5
LY = 64
TAU = 64
SITES = 4096
REPS = 20


def pairing(key):
    pick_key = jax.random.fold_in(key, 21)
    flag_key = jax.random.fold_in(key, 22)
    index = jnp.arange(REPS, dtype=jnp.int32)
    place = index % REP_DEV
    boundary = (place == REP_DEV - 1) & (index + 1 < REPS)
    inner = (place >= 1) & (place <= REP_DEV - 3)
    coins = jax.random.randint(pick_key, (REPS,), 0, 2, dtype=jnp.int32)
    wanted = inner & (coins == 1)
    wanted_before = jnp.concatenate([jnp.zeros((1,), dtype=bool), wanted[:-1]])
    chosen = boundary | wanted & jnp.logical_not(wanted_before)
    chosen_before = jnp.concatenate([jnp.zeros((1,), dtype=bool), chosen[:-1]])
    flags = jax.random.randint(flag_key, (REPS,), 0, 4, dtype=jnp.int32)
    edge_accept = jnp.where(boundary, 1, jnp.where(flags >= 1, 1, 0)).astype(jnp.int32)
    accept_before = jnp.concatenate([jnp.zeros((1,), dtype=jnp.int32), edge_accept[:-1]])
    partner = jnp.where(chosen, index + 1, jnp.where(chosen_before, index - 1, index))
    accept = jnp.where(chosen, edge_accept, jnp.where(chosen_before, accept_before, 0))
    return (partner.astype(jnp.int32), accept.astype(jnp.int32))


def draw_partner(key, part):
    return pairing(key)[0]


def draw_accept(key, part):
    return pairing(key)[1]


def plant(array, stream_key, least, high):
    shape = array.shape
    spot = [jax.random.randint(jax.random.fold_in(stream_key, axis), (), 0, shape[axis]) for axis in range(len(shape))]
    array = array.at[tuple(spot)].set(least)
    longest = shape.index(max(shape))
    spot[longest] = (spot[longest] + 1) % shape[longest]
    return array.at[tuple(spot)].set(high)


def block_levels(key, extent, shards, smallest, largest):
    factor_of, own = 1.0, jax.random.fold_in(key, 6)
    for dim, shards_of in shards:
        heights = jnp.exp(jax.random.uniform(jax.random.fold_in(own, dim), (shards_of,), jnp.float32, smallest / len(shards), largest / len(shards)))
        factor_of = factor_of * jnp.repeat(heights, extent[dim] // shards_of).reshape([-1 if axis == dim else 1 for axis in range(len(extent))])
    return factor_of


def centred(rng, extent, spread, reach, cuts=(), kind=jnp.bfloat16):
    values = spread * jax.random.normal(rng, extent, jnp.float32)
    if cuts:
        values = values * block_levels(rng, extent, cuts, -0.22, 0.18)
    return jnp.clip(values, -reach, reach).astype(kind)


def setup_inputs(seed: int = 0) -> dict:
    arg_keys = jax.random.split(jax.random.key(seed), 9)
    spins = centred(arg_keys[0], (REPS, 3, TAU, SITES), 0.6, 4.0, ((0, 4), (2, 4), (3, 2)), jnp.float32)
    bond_right = centred(arg_keys[1], (SITES,), 1.0, 4.0, ((0, 2),), jnp.float32)
    bond_down = centred(arg_keys[2], (SITES,), 1.0, 4.0, ((0, 2),), jnp.float32)
    betas = jnp.clip(jnp.exp(math.log(2.0) - 2.3025851 * jax.random.uniform(arg_keys[3], (REPS,), jnp.float32) ** block_levels(arg_keys[3], (REPS,), ((0, 4),), -0.2, 0.2)), 0.2, 2.0)
    time_coupling = jnp.clip(jnp.exp(math.log(1.0) - 2.3025851 * jax.random.uniform(arg_keys[4], (REPS,), jnp.float32) ** block_levels(arg_keys[4], (REPS,), ((0, 4),), -0.2, 0.2)), 0.1, 1.0)
    thresholds = plant(jax.random.randint(arg_keys[5], (2, REPS, TAU, SITES), 0, 8192), jax.random.fold_in(arg_keys[5], 1), 0, 8191).astype(jnp.int32)
    partner = draw_partner(jax.random.fold_in(arg_keys[8], 71), 0)
    accept = draw_accept(jax.random.fold_in(arg_keys[8], 71), 0)
    return dict(spins=spins, bond_right=bond_right, bond_down=bond_down, betas=betas, time_coupling=time_coupling, thresholds=thresholds, partner=partner, accept=accept)


def reference(spins, bond_right, bond_down, betas, time_coupling, thresholds, partner, accept):
    flat = jnp.arange(SITES)
    column = flat % LY
    row = flat // LY
    level = jnp.arange(TAU)
    parity = (row[None, :] + column[None, :] + level[:, None]) % 2
    bond_up = jnp.roll(bond_down, LY)
    bond_left = jnp.where(column == 0, jnp.roll(bond_right, -(LY - 1)), jnp.roll(bond_right, 1))
    beta_col = betas[:, None, None, None]
    coupling_col = time_coupling[:, None, None, None]
    state = spins
    for half in range(2):
        right = jnp.where(column == LY - 1, jnp.roll(state, LY - 1, axis=3), jnp.roll(state, -1, axis=3))
        left = jnp.where(column == 0, jnp.roll(state, -(LY - 1), axis=3), jnp.roll(state, 1, axis=3))
        down = jnp.roll(state, -LY, axis=3)
        upper = jnp.roll(state, LY, axis=3)
        field_space = bond_down * down + bond_up * upper + bond_right * right + bond_left * left
        later = jnp.roll(state, -1, axis=2)
        earlier = jnp.roll(state, 1, axis=2)
        field = beta_col * field_space + coupling_col * (later + earlier)
        weight = (thresholds[half].astype(jnp.float32) + 0.5) / 8192.0
        moved = state + weight[:, None] * field
        fresh = moved / jnp.sqrt(0.25 + lax.optimization_barrier(jnp.sum(moved * moved, axis=1, keepdims=True)))
        state = jnp.where(parity == half, fresh, state)
    right = jnp.where(column == LY - 1, jnp.roll(state, LY - 1, axis=3), jnp.roll(state, -1, axis=3))
    down = jnp.roll(state, -LY, axis=3)
    bonds = bond_down * lax.optimization_barrier(jnp.sum(state * down, axis=1)) + bond_right * lax.optimization_barrier(jnp.sum(state * right, axis=1))
    energy = -lax.optimization_barrier(jnp.sum(bonds, axis=-1)) / SITES
    source = jnp.where(accept == 1, partner, jnp.arange(REPS).astype(jnp.int32)).astype(jnp.int32)
    return (state[source], energy[source])
```

```python
import functools

import jax
import jax.numpy as jnp
from jax import lax
from jax.experimental import pallas as pl
from jax.experimental.pallas import tpu as pltpu
from jax.sharding import PartitionSpec as P

LY = 64
W = 2 * LY
MESH = pl.DeviceIdType.MESH


def kernel(
    sizes,
    betas, tcs, partner, accept, bond_right, bond_down, spins, thr,
    out, out_e,
    S, F, TH, OUT, HS, HT, ET, BO, BDS, BDH, CE, RC, EA, ER, EN,
    load_sem, halo_send, halo_recv, bond_sem, rep_send, rep_recv,
    en_send, en_recv, er_send, er_recv, out_sem,
):
    nrep, ntm, nsp = sizes
    R, C, T, L = S.shape
    NJ = L // W
    total = L * nsp
    ri, ti, si = lax.axis_index("rep"), lax.axis_index("tm"), lax.axis_index("space")
    has_low = ri > 0
    has_up = ri < nrep - 1
    t_prev, t_next = lax.rem(ti + ntm - 1, ntm), lax.rem(ti + 1, ntm)
    s_prev, s_next = lax.rem(si + nsp - 1, nsp), lax.rem(si + 1, nsp)
    r_up, r_low = lax.rem(ri + 1, nrep), lax.rem(ri + nrep - 1, nrep)

    def order(i):
        return lax.rem(i + R - 1, R)

    def loads(r):
        return (
            pltpu.make_async_copy(spins.at[r], S.at[r], load_sem.at[0, r]),
            pltpu.make_async_copy(thr.at[:, r], TH.at[:, r], load_sem.at[1, r]),
        )

    for i in range(R):
        a, b = loads((i + R - 1) % R)
        a.start()
        b.start()

    barrier = pltpu.get_barrier_semaphore()

    def greet(dev):
        pl.semaphore_signal(barrier, inc=1, device_id=dev, device_id_type=MESH)

    greet((ri, t_prev, si))
    greet((ri, t_next, si))
    for k in range(1, nsp):
        greet((ri, ti, lax.rem(si + k, nsp)))

    @pl.when(has_low)
    def _():
        for k in range(nsp):
            greet((r_low, ti, lax.rem(si + k, nsp)))

    @pl.when(has_up)
    def _():
        for k in range(nsp):
            greet((r_up, ti, lax.rem(si + k, nsp)))

    def halo(p, k, r):
        if k == 0:
            src, dst, dev = ET.at[p, 0, r], HT.at[p, 1, r], (ri, t_prev, si)
        elif k == 1:
            src, dst, dev = ET.at[p, 1, r], HT.at[p, 0, r], (ri, t_next, si)
        else:
            base = spins if p == 0 else S
            lo = 0 if k == 2 else L - W
            src = base.at[r, :, :, pl.ds(lo, W)]
            if k == 2:
                dst, dev = HS.at[p, 1, r], (ri, ti, s_prev)
            else:
                dst, dev = HS.at[p, 0, r], (ri, ti, s_next)
        return pltpu.make_async_remote_copy(
            src, dst, halo_send.at[p, k, r], halo_recv.at[p, k, r],
            device_id=dev, device_id_type=MESH,
        )

    def rep_copy(p, up):
        u = 1 if up else 0
        return pltpu.make_async_remote_copy(
            CE.at[u, p], RC.at[u, p], rep_send.at[u, p], rep_recv.at[u, p],
            device_id=(r_up if up else r_low, ti, si), device_id_type=MESH,
        )

    def en_copy(k, r):
        return pltpu.make_async_remote_copy(
            EA.at[0, r], EA.at[k, r], en_send.at[k, r], en_recv.at[k, r],
            device_id=(ri, ti, lax.rem(si + k, nsp)), device_id_type=MESH,
        )

    def er_copy(k, up):
        u = 1 if up else 0
        return pltpu.make_async_remote_copy(
            EA.at[0, R - 1 if up else 0], ER.at[u, k], er_send.at[u, k], er_recv.at[u, k],
            device_id=(r_up if up else r_low, ti, lax.rem(si + k, nsp)), device_id_type=MESH,
        )

    bond_copy = pltpu.make_async_remote_copy(
        BDS, BDH, bond_sem.at[0], bond_sem.at[1], device_id=(ri, ti, s_next), device_id_type=MESH
    )

    lane = lax.broadcasted_iota(jnp.int32, (8, W), 1)
    sub8 = lax.broadcasted_iota(jnp.int32, (8, W), 0)
    lane1 = lax.broadcasted_iota(jnp.int32, (T, W), 1)
    sub = lax.broadcasted_iota(jnp.int32, (T, W), 0)
    first_row = si * (L // LY)
    first_slice = ti * T
    lo8 = lane < LY
    lo_half = lane1 < LY
    col0 = lane1 % LY == 0
    col_last = lane1 % LY == LY - 1
    t_first = sub == 0
    t_last = sub == T - 1
    even = (lane1 // LY + lane1 % LY + sub + first_row + first_slice) % 2 == 0
    even8 = (lane // LY + lane % LY + sub8 + first_row + first_slice) % 2 == 0

    def row(ref, j):
        return jnp.broadcast_to(ref[pl.ds(j * W, W)].reshape(1, W), (8, W))

    BDS[...] = row(bond_down, NJ - 1)
    count = 2 + (nsp - 1) + nsp * (has_low.astype(jnp.int32) + has_up.astype(jnp.int32))
    pl.semaphore_wait(barrier, count)

    bond_copy.start()
    for i in range(R):
        for k in (2, 3):
            halo(0, k, (i + R - 1) % R).start()

    def edges(i, carry):
        r = order(i)
        loads(r)[0].wait()
        for c in range(C):
            ET[0, 0, r, c] = S[r, c, 0:1, :]
            ET[0, 1, r, c] = S[r, c, T - 1 : T, :]
        halo(0, 0, r).start()
        halo(0, 1, r).start()
        return carry

    lax.fori_loop(0, R, edges, 0)

    bond_copy.wait()
    prev_rot = pltpu.roll(BDH[...], LY, 1)
    for j in range(NJ):
        bd = row(bond_down, j)
        br = row(bond_right, j)
        rot = pltpu.roll(bd, LY, 1)
        BO[0, :, pl.ds(j * W, W)] = bd
        BO[1, :, pl.ds(j * W, W)] = jnp.where(lo8, prev_rot, rot)
        BO[2, :, pl.ds(j * W, W)] = br
        rot_r = pltpu.roll(br, LY, 1)
        BO[3, :, pl.ds(j * W, W)] = pltpu.roll(jnp.where(lane % LY == LY - 1, rot_r, br), 1, 1)
        prev_rot = rot

    def tall(x):
        return jnp.concatenate([x] * (T // 8), axis=0)

    def sweep(p, r, pack_to):
        beta = betas[r]
        tc = tcs[r]
        rots = {}

        def rot(j):
            if j not in rots:
                if j < 0:
                    rots[j] = [pltpu.roll(HS[p, 0, r, c], LY, 1) for c in range(C)]
                elif j >= NJ:
                    rots[j] = [pltpu.roll(HS[p, 1, r, c], LY, 1) for c in range(C)]
                else:
                    rots[j] = [pltpu.roll(S[r, c, :, pl.ds(j * W, W)], LY, 1) for c in range(C)]
            return rots[j]

        acc = jnp.zeros((T, W), jnp.float32)
        for j in range(NJ):
            at = pl.ds(j * W, W)
            before, here, after = rot(j - 1), rot(j), rot(j + 1)
            bd, bu, br, bl = (tall(BO[q, :, at]) for q in range(4))
            weight = (TH[p, r, :, at].astype(jnp.float32) + 0.5) * (1.0 / 8192.0)
            old, fields, moved = [], [], []
            for c in range(C):
                s = S[r, c, :, at]
                down = jnp.where(lo_half, here[c], after[c])
                up = jnp.where(lo_half, before[c], here[c])
                right = pltpu.roll(jnp.where(col0, here[c], s), W - 1, 1)
                left = pltpu.roll(jnp.where(col_last, here[c], s), 1, 1)
                fs = bd * down + bu * up + br * right + bl * left
                later = jnp.where(t_last, HT[p, 1, r, c, :, at], pltpu.roll(s, T - 1, 0))
                earlier = jnp.where(t_first, HT[p, 0, r, c, :, at], pltpu.roll(s, 1, 0))
                field = beta * fs + tc * (later + earlier)
                old.append(s)
                fields.append(fs)
                moved.append(s + weight * field)
            norm = lax.rsqrt(0.25 + (moved[0] * moved[0] + moved[1] * moved[1] + moved[2] * moved[2]))
            dot = None
            for c in range(C):
                fresh = moved[c] * norm
                if p == 0:
                    new = jnp.where(even, fresh, old[c])
                    S[r, c, :, at] = new
                    ET[1, 0, r, c, :, at] = new[0:1]
                    ET[1, 1, r, c, :, at] = new[T - 1 : T]
                else:
                    new = jnp.where(even, old[c], fresh)
                    F[r, c, :, at] = new
                    term = fresh * fields[c]
                    dot = term if dot is None else dot + term
                if pack_to is not None:
                    for b in range(T // 16):
                        a0 = new[16 * b : 16 * b + 8]
                        a1 = pltpu.roll(new[16 * b + 8 : 16 * b + 16], 1, 0)
                        kept = jnp.where(even8, a0, a1) if p == 0 else jnp.where(even8, a1, a0)
                        CE[pack_to, p, c, pl.ds(8 * b, 8), at] = kept
            if p == 1:
                acc = acc + jnp.where(even, 0.0, dot)
            del rots[j - 1]
        if p == 1:
            EA[0, r] = acc

    def halo_wait(p, r):
        for k in range(4):
            halo(p, k, r).wait_recv()

    def after_first(r):
        for k in range(4):
            halo(1, k, r).start()

    def first(r, pack_to):
        loads(r)[1].wait()
        halo_wait(0, r)
        sweep(0, r, pack_to)
        after_first(r)

    def edge_first(i, carry):
        r = order(i)
        first(r, 1 - i)

        @pl.when((i == 0) & has_up)
        def _():
            rep_copy(0, True).start()

        @pl.when((i == 1) & has_low)
        def _():
            rep_copy(0, False).start()

        return carry

    def inner_first(r, carry):
        first(r, None)
        return carry

    lax.fori_loop(0, 2, edge_first, 0)
    lax.fori_loop(1, R - 1, inner_first, 0)

    def second(r, pack_to):
        halo_wait(1, r)
        sweep(1, r, pack_to)
        for k in range(1, nsp):
            en_copy(k, r).start()

    def edge_second(i, carry):
        r = order(i)
        second(r, 1 - i)

        @pl.when((i == 0) & has_up)
        def _():
            for k in range(nsp):
                er_copy(k, True).start()
            rep_copy(1, True).start()

        @pl.when((i == 1) & has_low)
        def _():
            for k in range(nsp):
                er_copy(k, False).start()
            rep_copy(1, False).start()

        return carry

    def inner_second(r, carry):
        second(r, None)
        return carry

    lax.fori_loop(0, 2, edge_second, 0)
    lax.fori_loop(1, R - 1, inner_second, 0)

    def source(r):
        src = jnp.where(accept[r] == 1, partner[r] - ri * R, r)
        return jnp.clip(src, 0, R - 1)

    def put(r, src):
        for c in range(C):
            OUT[r, c] = F[src, c]

    def write(r):
        return pltpu.make_async_copy(OUT.at[r], out.at[r], out_sem.at[r])

    def inner_put(r, carry):
        put(r, source(r))
        write(r).start()
        return carry

    lax.fori_loop(1, R - 1, inner_put, 0)

    def unpack(u, r):
        for c in range(C):
            for j in range(NJ):
                at = pl.ds(j * W, W)
                for b in range(T // 16):
                    e = RC[u, 0, c, pl.ds(8 * b, 8), at]
                    o = RC[u, 1, c, pl.ds(8 * b, 8), at]
                    OUT[r, c, pl.ds(16 * b, 8), at] = jnp.where(even8, e, o)
                    OUT[r, c, pl.ds(16 * b + 8, 8), at] = pltpu.roll(jnp.where(even8, o, e), 7, 0)

    def lines(a):
        ones = jnp.ones((8, W), jnp.float32)
        sums = lax.dot_general(
            ones, a, (((1,), (1,)), ((), ())),
            precision=lax.Precision.HIGHEST, preferred_element_type=jnp.float32,
        )
        return -sums * (1.0 / total)

    for r in range(R):
        for k in range(1, nsp):
            en_copy(k, r).wait()
        a = EA[0, r]
        for k in range(1, nsp):
            a = a + EA[k, r]
        EN[r] = lines(a)

    for r in range(R):
        out_e[pl.ds(r, 1), :] = EN[source(r)][0:1]

    def edge_sum(u):
        a = ER[u, 0]
        for k in range(1, nsp):
            a = a + ER[u, k]
        return lines(a)[0:1]

    @pl.when(has_low)
    def _():
        for k in range(nsp):
            er_copy(k, True).wait_recv()
        out_e[pl.ds(0, 1), :] = edge_sum(1)
        rep_copy(0, True).wait_recv()
        rep_copy(1, True).wait_recv()
        unpack(1, 0)

    @pl.when(jnp.logical_not(has_low))
    def _():
        put(0, source(0))

    write(0).start()

    @pl.when(has_up)
    def _():
        for k in range(nsp):
            er_copy(k, False).wait_recv()
        out_e[pl.ds(R - 1, 1), :] = edge_sum(0)
        rep_copy(0, False).wait_recv()
        rep_copy(1, False).wait_recv()
        unpack(0, R - 1)

    @pl.when(jnp.logical_not(has_up))
    def _():
        put(R - 1, source(R - 1))

    write(R - 1).start()

    def drain(r, carry):
        for p in range(2):
            for k in range(4):
                halo(p, k, r).wait_send()
        write(r).wait()
        return carry

    lax.fori_loop(0, R, drain, 0)

    def sent(up):
        for k in range(nsp):
            er_copy(k, up).wait_send()
        for p in range(2):
            rep_copy(p, up).wait_send()

    pl.when(has_up)(lambda: sent(True))
    pl.when(has_low)(lambda: sent(False))


def on_device(sizes, spins, bond_right, bond_down, betas, time_coupling, thresholds, partner, accept):
    R, C, T, L = spins.shape
    nsp = sizes[2]
    f32 = jnp.float32
    vm, sm, any_ = (pl.BlockSpec(memory_space=m) for m in (pltpu.VMEM, pltpu.SMEM, pl.ANY))
    dma = pltpu.SemaphoreType.DMA
    return pl.pallas_call(
        functools.partial(kernel, sizes),
        out_shape=(
            jax.ShapeDtypeStruct((R, C, T, L), f32),
            jax.ShapeDtypeStruct((R, T), f32),
        ),
        in_specs=[sm, sm, sm, sm, vm, vm, any_, any_],
        out_specs=(any_, vm),
        scratch_shapes=[
            pltpu.VMEM((R, C, T, L), f32),
            pltpu.VMEM((R, C, T, L), f32),
            pltpu.VMEM((2, R, T, L), jnp.int32),
            pltpu.VMEM((R, C, T, L), f32),
            pltpu.VMEM((2, 2, R, C, T, W), f32),
            pltpu.VMEM((2, 2, R, C, 1, L), f32),
            pltpu.VMEM((2, 2, R, C, 1, L), f32),
            pltpu.VMEM((4, 8, L), f32),
            pltpu.VMEM((8, W), f32),
            pltpu.VMEM((8, W), f32),
            pltpu.VMEM((2, 2, C, T // 2, L), f32),
            pltpu.VMEM((2, 2, C, T // 2, L), f32),
            pltpu.VMEM((nsp, R, T, W), f32),
            pltpu.VMEM((2, nsp, T, W), f32),
            pltpu.VMEM((R, 8, T), f32),
            dma((2, R)),
            dma((2, 4, R)),
            dma((2, 4, R)),
            dma((2,)),
            dma((2, 2)),
            dma((2, 2)),
            dma((nsp, R)),
            dma((nsp, R)),
            dma((2, nsp)),
            dma((2, nsp)),
            dma((R,)),
        ],
        compiler_params=pltpu.CompilerParams(
            collective_id=0, has_side_effects=True, vmem_limit_bytes=56 * 1024 * 1024
        ),
        name="sweep_exchange",
    )(betas, time_coupling, partner, accept, bond_right, bond_down, spins, thresholds)


def solution(mesh):
    placed = (
        P("rep", None, "tm", "space"),
        P("space"),
        P("space"),
        P("rep"),
        P("rep"),
        P(None, "rep", "tm", "space"),
        P("rep"),
        P("rep"),
    )
    sizes = (mesh.shape["rep"], mesh.shape["tm"], mesh.shape["space"])
    return jax.shard_map(
        functools.partial(on_device, sizes),
        mesh=mesh,
        in_specs=placed,
        out_specs=(P("rep", None, "tm", "space"), P("rep", "tm")),
        check_vma=False,
    )
```

```python
import functools

import jax
import jax.numpy as jnp
from jax import lax
from jax.experimental import pallas as pl
from jax.experimental.pallas import tpu as pltpu
from jax.sharding import PartitionSpec as P

LY = 64
W = 2 * LY
MESH = pl.DeviceIdType.MESH


def kernel(
    sizes,
    betas, tcs, partner, accept, bond_right, bond_down, spins, thr,
    OUT, RC, out_e,
    S, F, TH, HS, HT, ET, BO, BDS, BDH, CE, EA, ER, EN,
    load_sem, halo_send, halo_recv, bond_sem, rep_send, rep_recv,
    en_send, en_recv, er_send, er_recv,
):
    nrep, ntm, nsp = sizes
    R, C, T, L = S.shape
    NJ = L // W
    total = L * nsp
    ri, ti, si = lax.axis_index("rep"), lax.axis_index("tm"), lax.axis_index("space")
    has_low = ri > 0
    has_up = ri < nrep - 1
    t_prev, t_next = lax.rem(ti + ntm - 1, ntm), lax.rem(ti + 1, ntm)
    s_prev, s_next = lax.rem(si + nsp - 1, nsp), lax.rem(si + 1, nsp)
    r_up, r_low = lax.rem(ri + 1, nrep), lax.rem(ri + nrep - 1, nrep)

    def order(i):
        return lax.rem(i + R - 1, R)

    def loads(r):
        return (
            pltpu.make_async_copy(spins.at[r], S.at[r], load_sem.at[0, r]),
            pltpu.make_async_copy(thr.at[:, r], TH.at[:, r], load_sem.at[1, r]),
        )

    for i in range(R):
        a, b = loads((i + R - 1) % R)
        a.start()
        b.start()

    barrier = pltpu.get_barrier_semaphore()

    def greet(dev):
        pl.semaphore_signal(barrier, inc=1, device_id=dev, device_id_type=MESH)

    greet((ri, t_prev, si))
    greet((ri, t_next, si))
    for k in range(1, nsp):
        greet((ri, ti, lax.rem(si + k, nsp)))

    @pl.when(has_low)
    def _():
        for k in range(nsp):
            greet((r_low, ti, lax.rem(si + k, nsp)))

    @pl.when(has_up)
    def _():
        for k in range(nsp):
            greet((r_up, ti, lax.rem(si + k, nsp)))

    def halo(p, k, r):
        if k == 0:
            src, dst, dev = ET.at[p, 0, r], HT.at[p, 1, r], (ri, t_prev, si)
        elif k == 1:
            src, dst, dev = ET.at[p, 1, r], HT.at[p, 0, r], (ri, t_next, si)
        else:
            base = spins if p == 0 else S
            lo = 0 if k == 2 else L - W
            src = base.at[r, :, :, pl.ds(lo, W)]
            if k == 2:
                dst, dev = HS.at[p, 1, r], (ri, ti, s_prev)
            else:
                dst, dev = HS.at[p, 0, r], (ri, ti, s_next)
        return pltpu.make_async_remote_copy(
            src, dst, halo_send.at[p, k, r], halo_recv.at[p, k, r],
            device_id=dev, device_id_type=MESH,
        )

    def rep_copy(p, up):
        u = 1 if up else 0
        return pltpu.make_async_remote_copy(
            CE.at[u, p], RC.at[u, p], rep_send.at[u, p], rep_recv.at[u, p],
            device_id=(r_up if up else r_low, ti, si), device_id_type=MESH,
        )

    def en_copy(k, r):
        return pltpu.make_async_remote_copy(
            EA.at[0, r], EA.at[k, r], en_send.at[k, r], en_recv.at[k, r],
            device_id=(ri, ti, lax.rem(si + k, nsp)), device_id_type=MESH,
        )

    def er_copy(k, up):
        u = 1 if up else 0
        return pltpu.make_async_remote_copy(
            EA.at[0, R - 1 if up else 0], ER.at[u, k], er_send.at[u, k], er_recv.at[u, k],
            device_id=(r_up if up else r_low, ti, lax.rem(si + k, nsp)), device_id_type=MESH,
        )

    bond_copy = pltpu.make_async_remote_copy(
        BDS, BDH, bond_sem.at[0], bond_sem.at[1], device_id=(ri, ti, s_next), device_id_type=MESH
    )

    lane = lax.broadcasted_iota(jnp.int32, (8, W), 1)
    sub8 = lax.broadcasted_iota(jnp.int32, (8, W), 0)
    lane1 = lax.broadcasted_iota(jnp.int32, (T, W), 1)
    sub = lax.broadcasted_iota(jnp.int32, (T, W), 0)
    first_row = si * (L // LY)
    first_slice = ti * T
    lo8 = lane < LY
    lo_half = lane1 < LY
    col0 = lane1 % LY == 0
    col_last = lane1 % LY == LY - 1
    t_first = sub == 0
    t_last = sub == T - 1
    even = (lane1 // LY + lane1 % LY + sub + first_row + first_slice) % 2 == 0
    even8 = (lane // LY + lane % LY + sub8 + first_row + first_slice) % 2 == 0

    def row(ref, j):
        return jnp.broadcast_to(ref[pl.ds(j * W, W)].reshape(1, W), (8, W))

    BDS[...] = row(bond_down, NJ - 1)
    count = 2 + (nsp - 1) + nsp * (has_low.astype(jnp.int32) + has_up.astype(jnp.int32))
    pl.semaphore_wait(barrier, count)

    bond_copy.start()
    for i in range(R):
        for k in (2, 3):
            halo(0, k, (i + R - 1) % R).start()

    def edges(i, carry):
        r = order(i)
        loads(r)[0].wait()
        for c in range(C):
            ET[0, 0, r, c] = S[r, c, 0:1, :]
            ET[0, 1, r, c] = S[r, c, T - 1 : T, :]
        halo(0, 0, r).start()
        halo(0, 1, r).start()
        return carry

    lax.fori_loop(0, R, edges, 0)

    bond_copy.wait()
    prev_rot = pltpu.roll(BDH[...], LY, 1)
    for j in range(NJ):
        bd = row(bond_down, j)
        br = row(bond_right, j)
        rot = pltpu.roll(bd, LY, 1)
        BO[0, :, pl.ds(j * W, W)] = bd
        BO[1, :, pl.ds(j * W, W)] = jnp.where(lo8, prev_rot, rot)
        BO[2, :, pl.ds(j * W, W)] = br
        rot_r = pltpu.roll(br, LY, 1)
        BO[3, :, pl.ds(j * W, W)] = pltpu.roll(jnp.where(lane % LY == LY - 1, rot_r, br), 1, 1)
        prev_rot = rot

    def tall(x):
        return jnp.concatenate([x] * (T // 8), axis=0)

    def sweep(p, r, pack_to):
        beta = betas[r]
        tc = tcs[r]
        rots = {}

        def rot(j):
            if j not in rots:
                if j < 0:
                    rots[j] = [pltpu.roll(HS[p, 0, r, c], LY, 1) for c in range(C)]
                elif j >= NJ:
                    rots[j] = [pltpu.roll(HS[p, 1, r, c], LY, 1) for c in range(C)]
                else:
                    rots[j] = [pltpu.roll(S[r, c, :, pl.ds(j * W, W)], LY, 1) for c in range(C)]
            return rots[j]

        acc = jnp.zeros((T, W), jnp.float32)
        for j in range(NJ):
            at = pl.ds(j * W, W)
            before, here, after = rot(j - 1), rot(j), rot(j + 1)
            bd, bu, br, bl = (tall(BO[q, :, at]) for q in range(4))
            weight = (TH[p, r, :, at].astype(jnp.float32) + 0.5) * (1.0 / 8192.0)
            old, fields, moved = [], [], []
            for c in range(C):
                s = S[r, c, :, at]
                down = jnp.where(lo_half, here[c], after[c])
                up = jnp.where(lo_half, before[c], here[c])
                right = pltpu.roll(jnp.where(col0, here[c], s), W - 1, 1)
                left = pltpu.roll(jnp.where(col_last, here[c], s), 1, 1)
                fs = bd * down + bu * up + br * right + bl * left
                later = jnp.where(t_last, HT[p, 1, r, c, :, at], pltpu.roll(s, T - 1, 0))
                earlier = jnp.where(t_first, HT[p, 0, r, c, :, at], pltpu.roll(s, 1, 0))
                field = beta * fs + tc * (later + earlier)
                old.append(s)
                fields.append(fs)
                moved.append(s + weight * field)
            norm = lax.rsqrt(0.25 + (moved[0] * moved[0] + moved[1] * moved[1] + moved[2] * moved[2]))
            dot = None
            for c in range(C):
                fresh = moved[c] * norm
                if p == 0:
                    new = jnp.where(even, fresh, old[c])
                    S[r, c, :, at] = new
                    ET[1, 0, r, c, :, at] = new[0:1]
                    ET[1, 1, r, c, :, at] = new[T - 1 : T]
                else:
                    new = jnp.where(even, old[c], fresh)
                    F[r, c, :, at] = new
                    term = fresh * fields[c]
                    dot = term if dot is None else dot + term
                if pack_to is not None:
                    for b in range(T // 16):
                        a0 = new[16 * b : 16 * b + 8]
                        a1 = pltpu.roll(new[16 * b + 8 : 16 * b + 16], 1, 0)
                        kept = jnp.where(even8, a0, a1) if p == 0 else jnp.where(even8, a1, a0)
                        CE[pack_to, p, c, pl.ds(8 * b, 8), at] = kept
            if p == 1:
                acc = acc + jnp.where(even, 0.0, dot)
            del rots[j - 1]
        if p == 1:
            EA[0, r] = acc

    def halo_wait(p, r):
        for k in range(4):
            halo(p, k, r).wait_recv()

    def after_first(r):
        for k in range(4):
            halo(1, k, r).start()

    def first(r, pack_to):
        loads(r)[1].wait()
        halo_wait(0, r)
        sweep(0, r, pack_to)
        after_first(r)

    def edge_first(i, carry):
        r = order(i)
        first(r, 1 - i)

        @pl.when((i == 0) & has_up)
        def _():
            rep_copy(0, True).start()

        @pl.when((i == 1) & has_low)
        def _():
            rep_copy(0, False).start()

        return carry

    def inner_first(r, carry):
        first(r, None)
        return carry

    lax.fori_loop(0, 2, edge_first, 0)
    lax.fori_loop(1, R - 1, inner_first, 0)

    def second(r, pack_to):
        halo_wait(1, r)
        sweep(1, r, pack_to)
        for k in range(1, nsp):
            en_copy(k, r).start()

    def edge_second(i, carry):
        r = order(i)
        second(r, 1 - i)

        @pl.when((i == 0) & has_up)
        def _():
            for k in range(nsp):
                er_copy(k, True).start()
            rep_copy(1, True).start()

        @pl.when((i == 1) & has_low)
        def _():
            for k in range(nsp):
                er_copy(k, False).start()
            rep_copy(1, False).start()

        return carry

    def inner_second(r, carry):
        second(r, None)
        return carry

    lax.fori_loop(0, 2, edge_second, 0)
    lax.fori_loop(1, R - 1, inner_second, 0)

    def source(r):
        src = jnp.where(accept[r] == 1, partner[r] - ri * R, r)
        return jnp.clip(src, 0, R - 1)

    def put(r, src):
        for c in range(C):
            OUT[r, c] = F[src, c]

    def inner_put(r, carry):
        put(r, source(r))
        return carry

    lax.fori_loop(1, R - 1, inner_put, 0)

    def lines(a):
        ones = jnp.ones((8, W), jnp.float32)
        sums = lax.dot_general(
            ones, a, (((1,), (1,)), ((), ())),
            precision=lax.Precision.HIGHEST, preferred_element_type=jnp.float32,
        )
        return -sums * (1.0 / total)

    for r in range(R):
        for k in range(1, nsp):
            en_copy(k, r).wait()
        a = EA[0, r]
        for k in range(1, nsp):
            a = a + EA[k, r]
        EN[r] = lines(a)

    for r in range(R):
        out_e[pl.ds(r, 1), :] = EN[source(r)][0:1]

    def edge_sum(u):
        a = ER[u, 0]
        for k in range(1, nsp):
            a = a + ER[u, k]
        return lines(a)[0:1]

    @pl.when(has_low)
    def _():
        for k in range(nsp):
            er_copy(k, True).wait_recv()
        out_e[pl.ds(0, 1), :] = edge_sum(1)
        rep_copy(0, True).wait_recv()
        rep_copy(1, True).wait_recv()

    @pl.when(jnp.logical_not(has_low))
    def _():
        put(0, source(0))

    @pl.when(has_up)
    def _():
        for k in range(nsp):
            er_copy(k, False).wait_recv()
        out_e[pl.ds(R - 1, 1), :] = edge_sum(0)
        rep_copy(0, False).wait_recv()
        rep_copy(1, False).wait_recv()

    @pl.when(jnp.logical_not(has_up))
    def _():
        put(R - 1, source(R - 1))

    def drain(r, carry):
        for p in range(2):
            for k in range(4):
                halo(p, k, r).wait_send()
        return carry

    lax.fori_loop(0, R, drain, 0)

    def sent(up):
        for k in range(nsp):
            er_copy(k, up).wait_send()
        for p in range(2):
            rep_copy(p, up).wait_send()

    pl.when(has_up)(lambda: sent(True))
    pl.when(has_low)(lambda: sent(False))


def store(sizes, kept, arrived, lines, out, out_e, edge, sem):
    R, C, T, L = kept.shape
    ri, ti, si = lax.axis_index("rep"), lax.axis_index("tm"), lax.axis_index("space")
    lane = lax.broadcasted_iota(jnp.int32, (8, W), 1)
    sub = lax.broadcasted_iota(jnp.int32, (8, W), 0)
    even = (lane // LY + lane % LY + sub + si * (L // LY) + ti * T) % 2 == 0

    def from_kept(r):
        return pltpu.make_async_copy(kept.at[r], out.at[r], sem.at[r])

    def from_edge(u, r):
        return pltpu.make_async_copy(edge.at[u], out.at[r], sem.at[r])

    for r in range(1, R - 1):
        from_kept(r).start()

    for u, r, met in ((1, 0, ri > 0), (0, R - 1, ri < sizes[0] - 1)):

        @pl.when(met)
        def _(u=u, r=r):
            for c in range(C):
                for j in range(L // W):
                    at = pl.ds(j * W, W)
                    for b in range(T // 16):
                        e = arrived[u, 0, c, pl.ds(8 * b, 8), at]
                        o = arrived[u, 1, c, pl.ds(8 * b, 8), at]
                        edge[u, c, pl.ds(16 * b, 8), at] = jnp.where(even, e, o)
                        edge[u, c, pl.ds(16 * b + 8, 8), at] = pltpu.roll(jnp.where(even, o, e), 7, 0)
            from_edge(u, r).start()

        @pl.when(jnp.logical_not(met))
        def _(r=r):
            from_kept(r).start()

    out_e[...] = lines[...]
    for r in range(R):
        from_kept(r).wait()


def on_device(sizes, spins, bond_right, bond_down, betas, time_coupling, thresholds, partner, accept):
    R, C, T, L = spins.shape
    nsp = sizes[2]
    f32 = jnp.float32
    vm, sm, any_ = (pl.BlockSpec(memory_space=m) for m in (pltpu.VMEM, pltpu.SMEM, pl.ANY))
    dma = pltpu.SemaphoreType.DMA
    kept, arrived, lines = pl.pallas_call(
        functools.partial(kernel, sizes),
        out_shape=(
            pltpu.VMEM((R, C, T, L), f32),
            pltpu.VMEM((2, 2, C, T // 2, L), f32),
            pltpu.VMEM((R, T), f32),
        ),
        in_specs=[sm, sm, sm, sm, vm, vm, any_, any_],
        out_specs=(vm, vm, vm),
        scratch_shapes=[
            pltpu.VMEM((R, C, T, L), f32),
            pltpu.VMEM((R, C, T, L), f32),
            pltpu.VMEM((2, R, T, L), jnp.int32),
            pltpu.VMEM((2, 2, R, C, T, W), f32),
            pltpu.VMEM((2, 2, R, C, 1, L), f32),
            pltpu.VMEM((2, 2, R, C, 1, L), f32),
            pltpu.VMEM((4, 8, L), f32),
            pltpu.VMEM((8, W), f32),
            pltpu.VMEM((8, W), f32),
            pltpu.VMEM((2, 2, C, T // 2, L), f32),
            pltpu.VMEM((nsp, R, T, W), f32),
            pltpu.VMEM((2, nsp, T, W), f32),
            pltpu.VMEM((R, 8, T), f32),
            dma((2, R)),
            dma((2, 4, R)),
            dma((2, 4, R)),
            dma((2,)),
            dma((2, 2)),
            dma((2, 2)),
            dma((nsp, R)),
            dma((nsp, R)),
            dma((2, nsp)),
            dma((2, nsp)),
        ],
        compiler_params=pltpu.CompilerParams(
            collective_id=0, has_side_effects=True, vmem_limit_bytes=56 * 1024 * 1024
        ),
        name="sweep_exchange",
    )(betas, time_coupling, partner, accept, bond_right, bond_down, spins, thresholds)
    return pl.pallas_call(
        functools.partial(store, sizes),
        out_shape=(
            jax.ShapeDtypeStruct((R, C, T, L), f32),
            jax.ShapeDtypeStruct((R, T), f32),
        ),
        in_specs=[vm, vm, vm],
        out_specs=(any_, vm),
        scratch_shapes=[pltpu.VMEM((2, C, T, L), f32), dma((R,))],
        compiler_params=pltpu.CompilerParams(vmem_limit_bytes=16 * 1024 * 1024),
        name="store_swapped",
    )(kept, arrived, lines)


def solution(mesh):
    placed = (
        P("rep", None, "tm", "space"),
        P("space"),
        P("space"),
        P("rep"),
        P("rep"),
        P(None, "rep", "tm", "space"),
        P("rep"),
        P("rep"),
    )
    sizes = (mesh.shape["rep"], mesh.shape["tm"], mesh.shape["space"])
    return jax.shard_map(
        functools.partial(on_device, sizes),
        mesh=mesh,
        in_specs=placed,
        out_specs=(P("rep", None, "tm", "space"), P("rep", "tm")),
        check_vma=False,
    )
```

```python
import functools

import jax
import jax.numpy as jnp
from jax import lax
from jax.experimental import pallas as pl
from jax.experimental.pallas import tpu as pltpu
from jax.sharding import PartitionSpec as P

LY = 64
W = 2 * LY
MESH = pl.DeviceIdType.MESH


def kernel(
    sizes,
    betas, tcs, partner, accept, bond_right, bond_down, spins, thr,
    OUT, RC, out_e,
    S, F, TH, HS, HT, ET, BO, BDS, BDH, CE, EA, ER, EN,
    load_sem, halo_send, halo_recv, bond_sem, rep_send, rep_recv,
    en_send, en_recv, er_send, er_recv,
):
    nrep, ntm, nsp = sizes
    R, C, T, L = S.shape
    NJ = L // W
    total = L * nsp
    ri, ti, si = lax.axis_index("rep"), lax.axis_index("tm"), lax.axis_index("space")
    has_low = ri > 0
    has_up = ri < nrep - 1
    t_prev, t_next = lax.rem(ti + ntm - 1, ntm), lax.rem(ti + 1, ntm)
    s_prev, s_next = lax.rem(si + nsp - 1, nsp), lax.rem(si + 1, nsp)
    r_up, r_low = lax.rem(ri + 1, nrep), lax.rem(ri + nrep - 1, nrep)

    def order(i):
        return lax.rem(i + R - 1, R)

    def loads(r):
        return (
            pltpu.make_async_copy(spins.at[r], S.at[r], load_sem.at[0, r]),
            pltpu.make_async_copy(thr.at[:, r], TH.at[:, r], load_sem.at[1, r]),
        )

    for i in range(R):
        a, b = loads((i + R - 1) % R)
        a.start()
        b.start()

    barrier = pltpu.get_barrier_semaphore()

    def greet(dev):
        pl.semaphore_signal(barrier, inc=1, device_id=dev, device_id_type=MESH)

    greet((ri, t_prev, si))
    greet((ri, t_next, si))
    for k in range(1, nsp):
        greet((ri, ti, lax.rem(si + k, nsp)))

    @pl.when(has_low)
    def _():
        for k in range(nsp):
            greet((r_low, ti, lax.rem(si + k, nsp)))

    @pl.when(has_up)
    def _():
        for k in range(nsp):
            greet((r_up, ti, lax.rem(si + k, nsp)))

    def halo(p, k, r):
        if k == 0:
            src, dst, dev = ET.at[p, 0, r], HT.at[p, 1, r], (ri, t_prev, si)
        elif k == 1:
            src, dst, dev = ET.at[p, 1, r], HT.at[p, 0, r], (ri, t_next, si)
        else:
            base = spins if p == 0 else S
            lo = 0 if k == 2 else L - W
            src = base.at[r, :, :, pl.ds(lo, W)]
            if k == 2:
                dst, dev = HS.at[p, 1, r], (ri, ti, s_prev)
            else:
                dst, dev = HS.at[p, 0, r], (ri, ti, s_next)
        return pltpu.make_async_remote_copy(
            src, dst, halo_send.at[p, k, r], halo_recv.at[p, k, r],
            device_id=dev, device_id_type=MESH,
        )

    def rep_copy(p, up):
        u = 1 if up else 0
        return pltpu.make_async_remote_copy(
            CE.at[u, p], RC.at[u, p], rep_send.at[u, p], rep_recv.at[u, p],
            device_id=(r_up if up else r_low, ti, si), device_id_type=MESH,
        )

    def en_copy(k, r):
        return pltpu.make_async_remote_copy(
            EA.at[0, r], EA.at[k, r], en_send.at[k, r], en_recv.at[k, r],
            device_id=(ri, ti, lax.rem(si + k, nsp)), device_id_type=MESH,
        )

    def er_copy(k, up):
        u = 1 if up else 0
        return pltpu.make_async_remote_copy(
            EA.at[0, R - 1 if up else 0], ER.at[u, k], er_send.at[u, k], er_recv.at[u, k],
            device_id=(r_up if up else r_low, ti, lax.rem(si + k, nsp)), device_id_type=MESH,
        )

    bond_copy = pltpu.make_async_remote_copy(
        BDS, BDH, bond_sem.at[0], bond_sem.at[1], device_id=(ri, ti, s_next), device_id_type=MESH
    )

    lane = lax.broadcasted_iota(jnp.int32, (8, W), 1)
    sub8 = lax.broadcasted_iota(jnp.int32, (8, W), 0)
    lane1 = lax.broadcasted_iota(jnp.int32, (T, W), 1)
    sub = lax.broadcasted_iota(jnp.int32, (T, W), 0)
    first_row = si * (L // LY)
    first_slice = ti * T
    lo8 = lane < LY
    lo_half = lane1 < LY
    col0 = lane1 % LY == 0
    col_last = lane1 % LY == LY - 1
    t_first = sub == 0
    t_last = sub == T - 1
    even = (lane1 // LY + lane1 % LY + sub + first_row + first_slice) % 2 == 0
    even8 = (lane // LY + lane % LY + sub8 + first_row + first_slice) % 2 == 0

    def row(ref, j):
        return jnp.broadcast_to(ref[pl.ds(j * W, W)].reshape(1, W), (8, W))

    BDS[...] = row(bond_down, NJ - 1)
    def edges(i, carry):
        r = order(i)
        loads(r)[0].wait()
        for c in range(C):
            for j in range(NJ):
                ET[0, 0, r, c, pl.ds(j, 1), :] = S[r, c, 0:1, pl.ds(j * W, W)]
                ET[0, 1, r, c, pl.ds(j, 1), :] = S[r, c, T - 1 : T, pl.ds(j * W, W)]
        halo(0, 0, r).start()
        halo(0, 1, r).start()
        return carry

    def edges_out(i, carry):
        r = order(i)
        for k in (2, 3):
            halo(0, k, r).start()
        return carry

    prev_rot = None
    for j in range(NJ):
        bd = row(bond_down, j)
        br = row(bond_right, j)
        rot = pltpu.roll(bd, LY, 1)
        BO[0, :, pl.ds(j * W, W)] = bd
        BO[1, :, pl.ds(j * W, W)] = rot if j == 0 else jnp.where(lo8, prev_rot, rot)
        BO[2, :, pl.ds(j * W, W)] = br
        rot_r = pltpu.roll(br, LY, 1)
        BO[3, :, pl.ds(j * W, W)] = pltpu.roll(jnp.where(lane % LY == LY - 1, rot_r, br), 1, 1)
        prev_rot = rot

    count = 2 + (nsp - 1) + nsp * (has_low.astype(jnp.int32) + has_up.astype(jnp.int32))
    pl.semaphore_wait(barrier, count)

    bond_copy.start()
    lax.fori_loop(0, R, edges_out, 0)
    lax.fori_loop(0, R, edges, 0)

    bond_copy.wait()
    BO[1, :, pl.ds(0, W)] = jnp.where(lo8, pltpu.roll(BDH[...], LY, 1), BO[1, :, pl.ds(0, W)])

    def tall(x):
        return jnp.concatenate([x] * (T // 8), axis=0)

    def sweep(p, r, pack_to):
        beta = betas[r]
        tc = tcs[r]
        rots = {}

        def rot(j):
            if j not in rots:
                if j < 0:
                    rots[j] = [pltpu.roll(HS[p, 0, r, c], LY, 1) for c in range(C)]
                elif j >= NJ:
                    rots[j] = [pltpu.roll(HS[p, 1, r, c], LY, 1) for c in range(C)]
                else:
                    rots[j] = [pltpu.roll(S[r, c, :, pl.ds(j * W, W)], LY, 1) for c in range(C)]
            return rots[j]

        acc = jnp.zeros((T, W), jnp.float32)
        for j in range(NJ):
            at = pl.ds(j * W, W)
            before, here, after = rot(j - 1), rot(j), rot(j + 1)
            bd, bu, br, bl = (tall(BO[q, :, at]) for q in range(4))
            weight = (TH[p, r, :, at].astype(jnp.float32) + 0.5) * (1.0 / 8192.0)
            old, fields, moved = [], [], []
            for c in range(C):
                s = S[r, c, :, at]
                down = jnp.where(lo_half, here[c], after[c])
                up = jnp.where(lo_half, before[c], here[c])
                right = pltpu.roll(jnp.where(col0, here[c], s), W - 1, 1)
                left = pltpu.roll(jnp.where(col_last, here[c], s), 1, 1)
                fs = bd * down + bu * up + br * right + bl * left
                later = jnp.where(t_last, HT[p, 1, r, c, pl.ds(j, 1), :], pltpu.roll(s, T - 1, 0))
                earlier = jnp.where(t_first, HT[p, 0, r, c, pl.ds(j, 1), :], pltpu.roll(s, 1, 0))
                field = beta * fs + tc * (later + earlier)
                old.append(s)
                fields.append(fs)
                moved.append(s + weight * field)
            norm = lax.rsqrt(0.25 + (moved[0] * moved[0] + moved[1] * moved[1] + moved[2] * moved[2]))
            dot = None
            for c in range(C):
                fresh = moved[c] * norm
                if p == 0:
                    new = jnp.where(even, fresh, old[c])
                    S[r, c, :, at] = new
                    ET[1, 0, r, c, pl.ds(j, 1), :] = new[0:1]
                    ET[1, 1, r, c, pl.ds(j, 1), :] = new[T - 1 : T]
                else:
                    new = jnp.where(even, old[c], fresh)
                    F[r, c, :, at] = new
                    term = fresh * fields[c]
                    dot = term if dot is None else dot + term
                if pack_to is not None:
                    for b in range(T // 16):
                        a0 = new[16 * b : 16 * b + 8]
                        a1 = pltpu.roll(new[16 * b + 8 : 16 * b + 16], 1, 0)
                        kept = jnp.where(even8, a0, a1) if p == 0 else jnp.where(even8, a1, a0)
                        CE[pack_to, p, c, pl.ds(8 * b, 8), at] = kept
            if p == 1:
                acc = acc + jnp.where(even, 0.0, dot)
            del rots[j - 1]
        if p == 1:
            EA[0, r] = acc

    def halo_wait(p, r):
        for k in range(4):
            halo(p, k, r).wait_recv()

    def after_first(r):
        for k in range(4):
            halo(1, k, r).start()

    def first(r, pack_to):
        loads(r)[1].wait()
        halo_wait(0, r)
        sweep(0, r, pack_to)
        after_first(r)

    def edge_first(i, carry):
        r = order(i)
        first(r, 1 - i)

        @pl.when((i == 0) & has_up)
        def _():
            rep_copy(0, True).start()

        @pl.when((i == 1) & has_low)
        def _():
            rep_copy(0, False).start()

        return carry

    def inner_first(r, carry):
        first(r, None)
        return carry

    lax.fori_loop(0, 2, edge_first, 0)
    lax.fori_loop(1, R - 1, inner_first, 0)

    def second(r, pack_to):
        halo_wait(1, r)
        sweep(1, r, pack_to)
        for k in range(1, nsp):
            en_copy(k, r).start()

    def edge_second(i, carry):
        r = order(i)
        second(r, 1 - i)

        @pl.when((i == 0) & has_up)
        def _():
            for k in range(nsp):
                er_copy(k, True).start()
            rep_copy(1, True).start()

        @pl.when((i == 1) & has_low)
        def _():
            for k in range(nsp):
                er_copy(k, False).start()
            rep_copy(1, False).start()

        return carry

    def inner_second(r, carry):
        second(r, None)
        return carry

    lax.fori_loop(0, 2, edge_second, 0)
    lax.fori_loop(1, R - 1, inner_second, 0)

    def source(r):
        src = jnp.where(accept[r] == 1, partner[r] - ri * R, r)
        return jnp.clip(src, 0, R - 1)

    def put(r, src):
        for c in range(C):
            OUT[r, c] = F[src, c]

    def inner_put(r, carry):
        put(r, source(r))
        return carry

    lax.fori_loop(1, R - 1, inner_put, 0)

    def lines(a):
        ones = jnp.ones((8, W), jnp.float32)
        sums = lax.dot_general(
            ones, a, (((1,), (1,)), ((), ())),
            precision=lax.Precision.HIGHEST, preferred_element_type=jnp.float32,
        )
        return -sums * (1.0 / total)

    for r in range(R):
        for k in range(1, nsp):
            en_copy(k, r).wait()
        a = EA[0, r]
        for k in range(1, nsp):
            a = a + EA[k, r]
        EN[r] = lines(a)

    for r in range(R):
        out_e[pl.ds(r, 1), :] = EN[source(r)][0:1]

    def edge_sum(u):
        a = ER[u, 0]
        for k in range(1, nsp):
            a = a + ER[u, k]
        return lines(a)[0:1]

    @pl.when(has_low)
    def _():
        for k in range(nsp):
            er_copy(k, True).wait_recv()
        out_e[pl.ds(0, 1), :] = edge_sum(1)
        rep_copy(0, True).wait_recv()
        rep_copy(1, True).wait_recv()

    @pl.when(jnp.logical_not(has_low))
    def _():
        put(0, source(0))

    @pl.when(has_up)
    def _():
        for k in range(nsp):
            er_copy(k, False).wait_recv()
        out_e[pl.ds(R - 1, 1), :] = edge_sum(0)
        rep_copy(0, False).wait_recv()
        rep_copy(1, False).wait_recv()

    @pl.when(jnp.logical_not(has_up))
    def _():
        put(R - 1, source(R - 1))

    def drain(r, carry):
        for p in range(2):
            for k in range(4):
                halo(p, k, r).wait_send()
        return carry

    lax.fori_loop(0, R, drain, 0)

    def sent(up):
        for k in range(nsp):
            er_copy(k, up).wait_send()
        for p in range(2):
            rep_copy(p, up).wait_send()

    pl.when(has_up)(lambda: sent(True))
    pl.when(has_low)(lambda: sent(False))


def store(sizes, kept, arrived, lines, out, out_e, edge, sem):
    R, C, T, L = kept.shape
    ri, ti, si = lax.axis_index("rep"), lax.axis_index("tm"), lax.axis_index("space")
    lane = lax.broadcasted_iota(jnp.int32, (8, W), 1)
    sub = lax.broadcasted_iota(jnp.int32, (8, W), 0)
    even = (lane // LY + lane % LY + sub + si * (L // LY) + ti * T) % 2 == 0

    def from_kept(r):
        return pltpu.make_async_copy(kept.at[r], out.at[r], sem.at[r])

    def from_edge(u, r):
        return pltpu.make_async_copy(edge.at[u], out.at[r], sem.at[r])

    for r in range(1, R - 1):
        from_kept(r).start()

    for u, r, met in ((1, 0, ri > 0), (0, R - 1, ri < sizes[0] - 1)):

        @pl.when(met)
        def _(u=u, r=r):
            for c in range(C):
                for j in range(L // W):
                    at = pl.ds(j * W, W)
                    for b in range(T // 16):
                        e = arrived[u, 0, c, pl.ds(8 * b, 8), at]
                        o = arrived[u, 1, c, pl.ds(8 * b, 8), at]
                        edge[u, c, pl.ds(16 * b, 8), at] = jnp.where(even, e, o)
                        edge[u, c, pl.ds(16 * b + 8, 8), at] = pltpu.roll(jnp.where(even, o, e), 7, 0)
            from_edge(u, r).start()

        @pl.when(jnp.logical_not(met))
        def _(r=r):
            from_kept(r).start()

    out_e[...] = lines[...]
    for r in range(R):
        from_kept(r).wait()


def on_device(sizes, spins, bond_right, bond_down, betas, time_coupling, thresholds, partner, accept):
    R, C, T, L = spins.shape
    nsp = sizes[2]
    f32 = jnp.float32
    vm, sm, any_ = (pl.BlockSpec(memory_space=m) for m in (pltpu.VMEM, pltpu.SMEM, pl.ANY))
    dma = pltpu.SemaphoreType.DMA
    kept, arrived, lines = pl.pallas_call(
        functools.partial(kernel, sizes),
        out_shape=(
            pltpu.VMEM((R, C, T, L), f32),
            pltpu.VMEM((2, 2, C, T // 2, L), f32),
            pltpu.VMEM((R, T), f32),
        ),
        in_specs=[sm, sm, sm, sm, vm, vm, any_, any_],
        out_specs=(vm, vm, vm),
        scratch_shapes=[
            pltpu.VMEM((R, C, T, L), f32),
            pltpu.VMEM((R, C, T, L), f32),
            pltpu.VMEM((2, R, T, L), jnp.int32),
            pltpu.VMEM((2, 2, R, C, T, W), f32),
            pltpu.VMEM((2, 2, R, C, L // W, W), f32),
            pltpu.VMEM((2, 2, R, C, L // W, W), f32),
            pltpu.VMEM((4, 8, L), f32),
            pltpu.VMEM((8, W), f32),
            pltpu.VMEM((8, W), f32),
            pltpu.VMEM((2, 2, C, T // 2, L), f32),
            pltpu.VMEM((nsp, R, T, W), f32),
            pltpu.VMEM((2, nsp, T, W), f32),
            pltpu.VMEM((R, 8, T), f32),
            dma((2, R)),
            dma((2, 4, R)),
            dma((2, 4, R)),
            dma((2,)),
            dma((2, 2)),
            dma((2, 2)),
            dma((nsp, R)),
            dma((nsp, R)),
            dma((2, nsp)),
            dma((2, nsp)),
        ],
        compiler_params=pltpu.CompilerParams(
            collective_id=0, has_side_effects=True, vmem_limit_bytes=56 * 1024 * 1024
        ),
        name="sweep_exchange",
    )(betas, time_coupling, partner, accept, bond_right, bond_down, spins, thresholds)
    return pl.pallas_call(
        functools.partial(store, sizes),
        out_shape=(
            jax.ShapeDtypeStruct((R, C, T, L), f32),
            jax.ShapeDtypeStruct((R, T), f32),
        ),
        in_specs=[vm, vm, vm],
        out_specs=(any_, vm),
        scratch_shapes=[pltpu.VMEM((2, C, T, L), f32), dma((R,))],
        compiler_params=pltpu.CompilerParams(vmem_limit_bytes=16 * 1024 * 1024),
        name="store_swapped",
    )(kept, arrived, lines)


def solution(mesh):
    placed = (
        P("rep", None, "tm", "space"),
        P("space"),
        P("space"),
        P("rep"),
        P("rep"),
        P(None, "rep", "tm", "space"),
        P("rep"),
        P("rep"),
    )
    sizes = (mesh.shape["rep"], mesh.shape["tm"], mesh.shape["space"])
    return jax.shard_map(
        functools.partial(on_device, sizes),
        mesh=mesh,
        in_specs=placed,
        out_specs=(P("rep", None, "tm", "space"), P("rep", "tm")),
        check_vma=False,
    )
```
